16 devices in a mesh: tp: 4 (over z, y), pp: 4 (over x, core).
Axes of the slice: x: 2, y: 2, z: 2, core: 2. Of those that a mesh axis runs over, the one named last changes fastest.
Arguments:
- x_micro: bfloat16 [6, 1, 1536, 2560], replicated
- ln1_gain: bfloat16 [4, 2560], P('pp')
- ln1_bias: bfloat16 [4, 2560], P('pp')
- w_qkv: bfloat16 [4, 2560, 32, 240], P('pp', None, 'tp')
- b_qkv: bfloat16 [4, 32, 240], P('pp', 'tp')
- w_dense: bfloat16 [4, 32, 80, 2560], P('pp', 'tp')
- b_dense: bfloat16 [4, 2560], P('pp')
- ln2_gain: bfloat16 [4, 2560], P('pp')
- ln2_bias: bfloat16 [4, 2560], P('pp')
- w_up: bfloat16 [4, 2560, 10240], P('pp', None, 'tp')
- b_up: bfloat16 [4, 10240], P('pp', 'tp')
- w_down: bfloat16 [4, 10240, 2560], P('pp', 'tp')
- b_down: bfloat16 [4, 2560], P('pp')
Outputs:
- output: bfloat16 [6, 1, 1536, 2560], replicated
All inputs are finite; a program needn't handle non-finite values.
Results may differ from the reference program's by a relative error of at most 0.0185461.
Values are sent between devices in bfloat16 or wider.
A program may use at most 1 GiB of HBM per device.

```python
import jax
import jax.numpy as jnp
from jax import lax

D = 2560
HEADS = 32
LAYERS = 4
MICRO = 6
BATCH = 1
SEQ = 1536
HEAD = D // HEADS
FFN = 4 * D
ROT = HEAD // 4


def setup_inputs(seed: int = 0) -> dict:
    key_list = jax.random.split(jax.random.key(seed), 13)

    def normal(sub_key, shape, scale):
        return jax.random.normal(sub_key, shape, jnp.float32) * scale

    qk_scale = jnp.concatenate([jnp.full((2 * HEAD,), 1.6, jnp.float32), jnp.ones((HEAD,), jnp.float32)])
    return {
        "x_micro": normal(key_list[0], (MICRO, BATCH, SEQ, D), 1.0).astype(jnp.bfloat16),
        "ln1_gain": (1.0 + normal(key_list[1], (LAYERS, D), 0.3)).astype(jnp.bfloat16),
        "ln1_bias": normal(key_list[2], (LAYERS, D), 0.3).astype(jnp.bfloat16),
        "w_qkv": (normal(key_list[3], (LAYERS, D, HEADS, 3 * HEAD), D ** -0.5) * qk_scale).astype(jnp.bfloat16),
        "b_qkv": normal(key_list[4], (LAYERS, HEADS, 3 * HEAD), 0.3).astype(jnp.bfloat16),
        "w_dense": normal(key_list[5], (LAYERS, HEADS, HEAD, D), D ** -0.5).astype(jnp.bfloat16),
        "b_dense": normal(key_list[6], (LAYERS, D), 0.3).astype(jnp.bfloat16),
        "ln2_gain": (1.0 + normal(key_list[7], (LAYERS, D), 0.3)).astype(jnp.bfloat16),
        "ln2_bias": normal(key_list[8], (LAYERS, D), 0.3).astype(jnp.bfloat16),
        "w_up": normal(key_list[9], (LAYERS, D, FFN), D ** -0.5).astype(jnp.bfloat16),
        "b_up": normal(key_list[10], (LAYERS, FFN), 0.3).astype(jnp.bfloat16),
        "w_down": normal(key_list[11], (LAYERS, FFN, D), FFN ** -0.5).astype(jnp.bfloat16),
        "b_down": normal(key_list[12], (LAYERS, D), 0.3).astype(jnp.bfloat16),
    }


def layer_norm(x_act, gain, bias):
    x_f32 = x_act.astype(jnp.float32)
    centered = x_f32 - jnp.mean(x_f32, axis=-1, keepdims=True)
    spread = jnp.mean(centered * centered, axis=-1, keepdims=True)
    normed = centered * lax.rsqrt(spread + 1e-5)
    return (normed * gain.astype(jnp.float32) + bias.astype(jnp.float32)).astype(jnp.bfloat16)


def rotary_tables():
    inv_freq = 1.0 / (10000.0 ** (jnp.arange(0, ROT, 2).astype(jnp.float32) / ROT))
    angles = jnp.arange(SEQ).astype(jnp.float32)[:, None] * inv_freq[None, :]
    angles = jnp.concatenate([angles, angles], axis=-1)
    return jnp.cos(angles), jnp.sin(angles)


def apply_rotary(heads_in, cos_tab, sin_tab):
    half_rot = ROT // 2
    rot_part = heads_in[..., :ROT].astype(jnp.float32)
    rotated = jnp.concatenate([-rot_part[..., half_rot:], rot_part[..., :half_rot]], axis=-1)
    mixed = rot_part * cos_tab[:, None, :] + rotated * sin_tab[:, None, :]
    return jnp.concatenate([mixed.astype(jnp.bfloat16), heads_in[..., ROT:]], axis=-1)


def neox_row(x_row, layer, cos_tab, sin_tab):
    ln_attn = layer_norm(x_row, layer["ln1_gain"], layer["ln1_bias"])
    qkv_proj = jnp.dot(ln_attn, layer["w_qkv"].reshape(D, HEADS * 3 * HEAD), preferred_element_type=jnp.float32)
    qkv_proj = (qkv_proj.reshape(SEQ, HEADS, 3 * HEAD) + layer["b_qkv"].astype(jnp.float32)).astype(jnp.bfloat16)
    query = apply_rotary(qkv_proj[..., :HEAD], cos_tab, sin_tab)
    key_rot = apply_rotary(qkv_proj[..., HEAD:2 * HEAD], cos_tab, sin_tab)
    values = qkv_proj[..., 2 * HEAD:]
    scores = jnp.einsum("qhd,khd->hqk", query.astype(jnp.float32), key_rot.astype(jnp.float32)) * HEAD ** -0.5
    causal = jnp.arange(SEQ)[:, None] >= jnp.arange(SEQ)[None, :]
    scores = jnp.where(causal[None], scores, -1e30)
    probs = jax.nn.softmax(scores, axis=-1).astype(jnp.bfloat16)
    context = jnp.einsum("hqk,khd->qhd", probs.astype(jnp.float32), values.astype(jnp.float32)).astype(jnp.bfloat16)
    attn_part = jnp.dot(context.reshape(SEQ, D), layer["w_dense"].reshape(D, D), preferred_element_type=jnp.float32)
    ln_mlp = layer_norm(x_row, layer["ln2_gain"], layer["ln2_bias"])
    hidden = jnp.dot(ln_mlp, layer["w_up"], preferred_element_type=jnp.float32) + layer["b_up"].astype(jnp.float32)
    hidden = jax.nn.gelu(hidden, approximate=False).astype(jnp.bfloat16)
    mlp_part = jnp.dot(hidden, layer["w_down"], preferred_element_type=jnp.float32)
    bias_sum = layer["b_dense"].astype(jnp.float32) + layer["b_down"].astype(jnp.float32)
    return (x_row.astype(jnp.float32) + bias_sum + attn_part + mlp_part).astype(jnp.bfloat16)


def reference(x_micro, ln1_gain, ln1_bias, w_qkv, b_qkv, w_dense, b_dense, ln2_gain, ln2_bias, w_up, b_up, w_down, b_down):
    cos_tab, sin_tab = rotary_tables()
    stacked = {
        "ln1_gain": ln1_gain, "ln1_bias": ln1_bias, "w_qkv": w_qkv, "b_qkv": b_qkv,
        "w_dense": w_dense, "b_dense": b_dense, "ln2_gain": ln2_gain, "ln2_bias": ln2_bias,
        "w_up": w_up, "b_up": b_up, "w_down": w_down, "b_down": b_down,
    }
    rows = x_micro.reshape(MICRO * BATCH, SEQ, D)

    def one_layer(carry, layer):
        return lax.map(lambda x_row: neox_row(x_row, layer, cos_tab, sin_tab), carry), None

    final, _ = lax.scan(one_layer, rows, stacked)
    return final.reshape(MICRO, BATCH, SEQ, D)
```

```python
import functools

import jax
import jax.numpy as jnp
from jax import lax
from jax.experimental import pallas as pl
from jax.experimental.pallas import tpu as pltpu
from jax.sharding import PartitionSpec as P

CHUNKS = 2
Q_BLOCK = 256
ROT_PAD = 32
LOG2E = 1.4426950408889634


def ln_kernel(stage_ref, first_ref, later_ref, gain1_ref, bias1_ref, gain2_ref, bias2_ref, attn_ref, mlp_ref):
    group = 16

    def run(source):
        def body(index, _):
            span = pl.ds(pl.multiple_of(index * group, group), group)
            x_f32 = source[span, :].astype(jnp.float32)
            centered = x_f32 - jnp.mean(x_f32, axis=-1, keepdims=True)
            spread = jnp.mean(centered * centered, axis=-1, keepdims=True)
            normed = centered * lax.rsqrt(spread + 1e-5)
            attn_ref[span, :] = (normed * gain1_ref[...] + bias1_ref[...]).astype(jnp.bfloat16)
            mlp_ref[span, :] = (normed * gain2_ref[...] + bias2_ref[...]).astype(jnp.bfloat16)
            return 0

        lax.fori_loop(0, attn_ref.shape[0] // group, body, 0, unroll=2)

    @pl.when(stage_ref[0] == 0)
    def _():
        run(first_ref.at[0])

    @pl.when(stage_ref[0] != 0)
    def _():
        run(later_ref)


def layer_norms(stage, slot, first, later, gain1, bias1, gain2, bias2):
    rows, width = later.shape
    block = 128
    scalars = jnp.stack([stage, slot]).astype(jnp.int32)
    vec = pl.BlockSpec((1, width), lambda j, s: (0, 0))
    return pl.pallas_call(
        ln_kernel,
        out_shape=[jax.ShapeDtypeStruct((rows, width), jnp.bfloat16)] * 2,
        grid_spec=pltpu.PrefetchScalarGridSpec(
            num_scalar_prefetch=1,
            grid=(rows // block,),
            in_specs=[
                pl.BlockSpec((1, block, width), lambda j, s: (s[1], jnp.where(s[0] == 0, j, 0), 0)),
                pl.BlockSpec((block, width), lambda j, s: (jnp.where(s[0] == 0, 0, j), 0)),
                vec, vec, vec, vec,
            ],
            out_specs=[pl.BlockSpec((block, width), lambda j, s: (j, 0))] * 2,
        ),
        cost_estimate=pl.CostEstimate(flops=rows * width * 600, bytes_accessed=rows * width * 6, transcendentals=0),
        name="layer_norms",
    )(scalars, first, later, gain1, bias1, gain2, bias2)


def rotate(x_t, swap, cos_t, sin_t):
    top = swap.shape[0]
    swapped = jnp.dot(swap, x_t, preferred_element_type=jnp.float32)
    mixed = x_t[:top].astype(jnp.float32) * cos_t + swapped * sin_t
    return jnp.concatenate([mixed, x_t[top:].astype(jnp.float32)], axis=0)


def attn_kernel(n_prev, *refs):
    if n_prev:
        q_ref, k_ref, v_ref, swap_ref, cos_ref, sin_ref, k_prev_ref, v_prev_ref, ctx_ref = refs
    else:
        q_ref, k_ref, v_ref, swap_ref, cos_ref, sin_ref, ctx_ref, k_out_ref = refs
    head_dim, rows = q_ref.shape[1:]
    scale = head_dim ** -0.5 * LOG2E
    q_t = rotate(q_ref[0], swap_ref[...], cos_ref[...], sin_ref[...]).astype(jnp.bfloat16)
    k_new = rotate(k_ref[0], swap_ref[...], cos_ref[...], sin_ref[...]).T.astype(jnp.bfloat16)
    if not n_prev:
        k_out_ref[0] = k_new
    causal = lax.broadcasted_iota(jnp.int32, (Q_BLOCK, Q_BLOCK), 0) <= lax.broadcasted_iota(jnp.int32, (Q_BLOCK, Q_BLOCK), 1)
    for block in range(rows // Q_BLOCK):
        lo, hi = block * Q_BLOCK, (block + 1) * Q_BLOCK
        q_blk = q_t[:, lo:hi]
        parts = []
        if n_prev:
            parts.append((k_prev_ref[0], v_prev_ref[0]))
        if lo:
            parts.append((k_new[:lo], v_ref[0, :, :lo]))
        parts.append((k_new[lo:hi], v_ref[0, :, lo:hi]))
        scores = [jnp.dot(k_part, q_blk, preferred_element_type=jnp.float32) * scale for k_part, _ in parts]
        scores[-1] = jnp.where(causal, scores[-1], -1e30)
        top = functools.reduce(jnp.maximum, [jnp.max(s, axis=0, keepdims=True) for s in scores])
        exps = [jnp.exp2(s - top) for s in scores]
        total = functools.reduce(jnp.add, [jnp.sum(e, axis=0, keepdims=True) for e in exps])
        inv = 1.0 / total
        ctx = None
        for e, (_, v_part) in zip(exps, parts):
            term = jnp.dot(v_part, (e * inv).astype(jnp.bfloat16), preferred_element_type=jnp.float32)
            ctx = term if ctx is None else ctx + term
        ctx_ref[0, :, lo:hi] = ctx.astype(jnp.bfloat16)


def attention(qkv_t, swap, cos_t, sin_t, previous):
    n_heads, head_dim, rows = qkv_t.shape[0] // 3, qkv_t.shape[1], qkv_t.shape[2]
    n_prev = previous[0].shape[1] if previous else 0
    part = lambda which: pl.BlockSpec((1, head_dim, rows), lambda h: (3 * h + which, 0, 0))
    table = pl.BlockSpec((ROT_PAD, rows), lambda h: (0, 0))
    whole = pl.BlockSpec(swap.shape, lambda h: (0, 0))
    in_specs = [part(0), part(1), part(2), whole, table, table]
    operands = [qkv_t, qkv_t, qkv_t, swap, cos_t, sin_t]
    out_shape = [jax.ShapeDtypeStruct((n_heads, head_dim, rows), jnp.bfloat16)]
    out_specs = [pl.BlockSpec((1, head_dim, rows), lambda h: (h, 0, 0))]
    if previous:
        in_specs += [pl.BlockSpec((1, n_prev, head_dim), lambda h: (h, 0, 0)), pl.BlockSpec((1, head_dim, n_prev), lambda h: (3 * h + 2, 0, 0))]
        operands += list(previous)
    else:
        out_shape.append(jax.ShapeDtypeStruct((n_heads, rows, head_dim), jnp.bfloat16))
        out_specs.append(pl.BlockSpec((1, rows, head_dim), lambda h: (h, 0, 0)))
    pairs = n_heads * rows * (n_prev + rows)
    return pl.pallas_call(
        functools.partial(attn_kernel, n_prev),
        out_shape=out_shape,
        grid=(n_heads,),
        in_specs=in_specs,
        out_specs=out_specs,
        cost_estimate=pl.CostEstimate(flops=pairs * 1000, bytes_accessed=n_heads * rows * 128 * 12, transcendentals=pairs),
        name="attention",
    )(*operands)


def qkv_kernel(w_ref, ln_ref, bias_ref, out_ref):
    acc = lax.dot_general(w_ref[...], ln_ref[...], (((1,), (1,)), ((), ())), preferred_element_type=jnp.float32)
    out_ref[...] = (acc + bias_ref[...]).astype(jnp.bfloat16)


def qkv_projection(w_t, ln, bias_t):
    features, width = w_t.shape
    rows = ln.shape[0]
    block = features // 4
    return pl.pallas_call(
        qkv_kernel,
        out_shape=jax.ShapeDtypeStruct((features, rows), jnp.bfloat16),
        grid=(features // block,),
        in_specs=[pl.BlockSpec((block, width), lambda j: (j, 0)), pl.BlockSpec((rows, width), lambda j: (0, 0)),
                  pl.BlockSpec((block, 1), lambda j: (j, 0))],
        out_specs=pl.BlockSpec((block, rows), lambda j: (j, 0)),
        cost_estimate=pl.CostEstimate(flops=2 * features * width * rows, bytes_accessed=2 * features * width, transcendentals=0),
        name="qkv_projection",
    )(w_t, ln, bias_t)


def up_kernel(ln_ref, w_ref, bias_ref, out_ref):
    hidden = jnp.dot(ln_ref[...], w_ref[...], preferred_element_type=jnp.float32) + bias_ref[...]
    out_ref[...] = (0.5 * hidden * (1.0 + lax.erf(hidden * (0.5 ** 0.5)))).astype(jnp.bfloat16)


def up_projection(ln, w_up, bias, part):
    rows, width = ln.shape
    inner = w_up.shape[1] // 2
    block = 256
    return pl.pallas_call(
        up_kernel,
        out_shape=jax.ShapeDtypeStruct((rows, inner), jnp.bfloat16),
        grid=(inner // block,),
        in_specs=[pl.BlockSpec((rows, width), lambda j: (0, 0)), pl.BlockSpec((width, block), lambda j: (0, j + part * (inner // block))),
                  pl.BlockSpec((1, block), lambda j: (0, j + part * (inner // block)))],
        out_specs=pl.BlockSpec((rows, block), lambda j: (0, j)),
        cost_estimate=pl.CostEstimate(flops=2 * inner * width * rows, bytes_accessed=2 * inner * width, transcendentals=0),
        name="up_projection",
    )(ln, w_up, bias)


def down_kernel(low_ref, high_ref, ctx_t_ref, w_low_ref, w_high_ref, w_dense_ref, out_ref, ctx_ref):
    @pl.when(pl.program_id(0) == 0)
    def _():
        ctx_ref[...] = ctx_t_ref[...].T

    attn = jnp.dot(ctx_ref[...], w_dense_ref[...], preferred_element_type=jnp.float32)
    low = jnp.dot(low_ref[...], w_low_ref[...], preferred_element_type=jnp.float32)
    high = jnp.dot(high_ref[...], w_high_ref[...], preferred_element_type=jnp.float32)
    out_ref[...] = (attn + (low + high)).astype(jnp.bfloat16)


def down_projection(low, high, ctx_t, w_down, w_dense):
    rows, inner = low.shape
    features, width = w_dense.shape
    block = 256
    return pl.pallas_call(
        down_kernel,
        out_shape=jax.ShapeDtypeStruct((rows, width), jnp.bfloat16),
        grid=(width // block,),
        in_specs=[pl.BlockSpec((rows, inner), lambda j: (0, 0)), pl.BlockSpec((rows, inner), lambda j: (0, 0)),
                  pl.BlockSpec((features, rows), lambda j: (0, 0)), pl.BlockSpec((inner, block), lambda j: (0, j)),
                  pl.BlockSpec((inner, block), lambda j: (1, j)), pl.BlockSpec((features, block), lambda j: (0, j))],
        out_specs=pl.BlockSpec((rows, block), lambda j: (0, j)),
        scratch_shapes=[pltpu.VMEM((rows, features), jnp.bfloat16)],
        cost_estimate=pl.CostEstimate(flops=2 * (2 * inner + features) * width * rows, bytes_accessed=2 * (2 * inner + features) * width, transcendentals=0),
        name="down_projection",
    )(low, high, ctx_t, w_down, w_down, w_dense)


def unwritten(shape):
    return pl.pallas_call(
        lambda out_ref: None,
        out_shape=jax.ShapeDtypeStruct(shape, jnp.bfloat16),
        out_specs=pl.BlockSpec(memory_space=pl.ANY),
        name="unwritten",
    )()


def store_kernel(sel_ref, held_ref, *refs):
    *cand_refs, out_ref, buf_ref, in_sem, out_sem = refs
    pieces, block = buf_ref.shape[:2]
    slot = sel_ref[1]

    def read(cand_ref, piece):
        return pltpu.make_async_copy(cand_ref.at[pl.ds(piece * block, block)], buf_ref.at[piece], in_sem.at[piece])

    def write(piece):
        return pltpu.make_async_copy(buf_ref.at[piece], out_ref.at[slot, pl.ds(piece * block, block)], out_sem.at[piece])

    for index, cand_ref in enumerate(cand_refs):
        @pl.when(sel_ref[0] == index)
        def _():
            for piece in range(pieces):
                read(cand_ref, piece).start()
    for piece in range(pieces):
        read(cand_refs[0], piece).wait()
        write(piece).start()
    for piece in range(pieces):
        write(piece).wait()


def store_final(result, which, slot, candidates):
    rows, width = candidates[0].shape
    pieces = 4
    hbm = pl.BlockSpec(memory_space=pltpu.HBM)
    scalars = jnp.stack([which, slot]).astype(jnp.int32)
    return pl.pallas_call(
        store_kernel,
        out_shape=jax.ShapeDtypeStruct(result.shape, result.dtype),
        in_specs=[pl.BlockSpec(memory_space=pltpu.SMEM)] + [hbm] * (1 + len(candidates)),
        out_specs=hbm,
        scratch_shapes=[pltpu.VMEM((pieces, rows // pieces, width), result.dtype),
                        pltpu.SemaphoreType.DMA((pieces,)), pltpu.SemaphoreType.DMA((pieces,))],
        input_output_aliases={1: 0},
        cost_estimate=pl.CostEstimate(flops=rows * width * 300, bytes_accessed=rows * width * 4, transcendentals=0),
        name="store_final",
    )(scalars, result, *candidates)


def rotary_tables(seq_len, rot_dims, head_dim):
    half = rot_dims // 2
    inv_freq = 1.0 / (10000.0 ** (jnp.arange(0, rot_dims, 2).astype(jnp.float32) / rot_dims))
    angles = inv_freq[:, None] * jnp.arange(seq_len).astype(jnp.float32)[None, :]
    spare = ROT_PAD - rot_dims
    cos_t = jnp.concatenate([jnp.cos(angles), jnp.cos(angles), jnp.ones((spare, seq_len), jnp.float32)])
    sin_t = jnp.concatenate([jnp.sin(angles), jnp.sin(angles), jnp.zeros((spare, seq_len), jnp.float32)])
    row = lax.broadcasted_iota(jnp.int32, (ROT_PAD, head_dim), 0)
    col = lax.broadcasted_iota(jnp.int32, (ROT_PAD, head_dim), 1)
    minus = jnp.logical_and(row < half, col == row + half)
    plus = jnp.logical_and(jnp.logical_and(row >= half, row < rot_dims), col == row - half)
    swap = jnp.where(plus, 1.0, jnp.where(minus, -1.0, 0.0)).astype(jnp.bfloat16)
    return swap, cos_t, sin_t


def solution(mesh):
    n_stages, n_tp = mesh.shape["pp"], mesh.shape["tp"]
    in_specs = (P(), P("pp", None), P("pp", None), P("pp", None, "tp", None), P("pp", "tp", None),
                P("pp", "tp", None, None), P("pp", None), P("pp", None), P("pp", None),
                P("pp", None, "tp"), P("pp", "tp"), P("pp", "tp", None), P("pp", None))

    def device_fn(x_micro, ln1_gain, ln1_bias, w_qkv, b_qkv, w_dense, b_dense, ln2_gain, ln2_bias, w_up, b_up, w_down, b_down):
        n_micro, _, seq_len, width = x_micro.shape
        n_heads, head_dim = w_dense.shape[1:3]
        rows = seq_len // CHUNKS
        quarter = rows // n_tp
        stage, tp_id = lax.axis_index("pp"), lax.axis_index("tp")
        x_chunks = x_micro.reshape(n_micro * CHUNKS, rows, width)
        norms = [v[:1].astype(jnp.float32) for v in (ln1_gain, ln1_bias, ln2_gain, ln2_bias)]
        bias_sum = b_dense[0].astype(jnp.float32) + b_down[0].astype(jnp.float32)
        w_qkv_t = w_qkv[0].transpose(1, 2, 0).reshape(n_heads * 3 * head_dim, width)
        b_qkv_t = b_qkv[0].reshape(n_heads * 3 * head_dim, 1).astype(jnp.float32)
        w_qkv_t, b_qkv_t = lax.optimization_barrier((w_qkv_t, b_qkv_t))
        w_out = w_dense[0].reshape(n_heads * head_dim, width)
        up_bias = b_up[:1].astype(jnp.float32)
        swap, cos_t, sin_t = rotary_tables(seq_len, head_dim // 4, head_dim)
        tables = [(cos_t[:, c * rows:(c + 1) * rows], sin_t[:, c * rows:(c + 1) * rows]) for c in range(CHUNKS)]
        tables = lax.optimization_barrier(tables)
        ring = [(s, (s + 1) % n_stages) for s in range(n_stages)]

        def norms_of(chunk, slot, gathered):
            where_from = slot * CHUNKS + chunk
            ln_attn, ln_mlp = layer_norms(stage, where_from, x_chunks, gathered, *norms)
            from_x = lax.dynamic_slice(x_chunks, (where_from, tp_id * quarter, 0), (1, quarter, width))[0]
            from_ring = lax.dynamic_slice(gathered, (tp_id * quarter, 0), (quarter, width))
            return ln_attn, ln_mlp, jnp.where(stage == 0, from_x, from_ring)

        def attend(chunk, ln_attn, previous):
            qkv_t = qkv_projection(w_qkv_t, ln_attn, b_qkv_t).reshape(3 * n_heads, head_dim, rows)
            if previous is None:
                ctx_t, keys = attention(qkv_t, swap, *tables[chunk], None)
                previous = (keys, qkv_t)
            else:
                ctx_t, = attention(qkv_t, swap, *tables[chunk], previous)
            return ctx_t.reshape(n_heads * head_dim, rows), previous

        def scatter(partial):
            return lax.psum_scatter(partial, "tp", scatter_dimension=0, tiled=True)

        def pass_on(summed, kept):
            out = (kept.astype(jnp.float32) + bias_sum + summed.astype(jnp.float32)).astype(jnp.bfloat16)
            return lax.ppermute(out, "pp", ring)

        def gather(out):
            return lax.all_gather(out, "tp", axis=0, tiled=True)

        def to_second(final):
            return lax.ppermute(final, "pp", [(0, 2)]), lax.ppermute(final, "pp", [(0, 1)])

        def to_third(far):
            return lax.ppermute(far, "pp", [(2, 3)])

        def half(chunk, slot, gathered, previous, partial_before, kept_before):
            summed = scatter(partial_before)
            far, near = to_second(gathered)
            ln_attn, ln_mlp, kept = norms_of(chunk, slot, gathered)
            ctx_t, previous = attend(chunk, ln_attn, previous)
            low = up_projection(ln_mlp, w_up[0], up_bias, 0)
            summed, far, near, ctx_t, low, ln_mlp = lax.optimization_barrier((summed, far, near, ctx_t, low, ln_mlp))
            passed = pass_on(summed, kept_before)
            farthest = to_third(far)
            high = up_projection(ln_mlp, w_up[0], up_bias, 1)
            passed, high = lax.optimization_barrier((passed, high))
            gathered_before = gather(passed)
            partial = down_projection(low, high, ctx_t, w_down[0], w_out)
            gathered_before, partial, farthest = lax.optimization_barrier((gathered_before, partial, farthest))
            return gathered_before, partial, kept, previous, (gathered, near, far, farthest)

        def tick(step, carry):
            gathered_a, partial_b, kept_b, result = carry
            slot = jnp.clip(step, 0, n_micro - 1)
            done = jnp.maximum(step - n_stages, 0)
            gathered_b, partial_a, kept_a, previous, finals = half(0, slot, gathered_a, None, partial_b, kept_b)
            result = store_final(result, stage, done * CHUNKS, finals)
            next_a, partial_b, kept_b, _, finals = half(1, slot, gathered_b, previous, partial_a, kept_a)
            result = store_final(result, stage, done * CHUNKS + 1, finals)
            return next_a, partial_b, kept_b, result

        start = (x_chunks[0], x_chunks[1], x_chunks[0, :quarter], unwritten(x_chunks.shape))
        last_a, partial_b, kept_b, result = lax.fori_loop(0, n_micro + n_stages - 1, tick, start)
        summed = scatter(partial_b)
        far_a, near_a = to_second(last_a)
        summed, far_a, near_a = lax.optimization_barrier((summed, far_a, near_a))
        out = (kept_b.astype(jnp.float32) + bias_sum + summed.astype(jnp.float32)).astype(jnp.bfloat16)
        at_first = lax.ppermute(out, "pp", [(n_stages - 1, 0)])
        at_third = lax.ppermute(out, "pp", [(n_stages - 1, 2)])
        farthest_a = to_third(far_a)
        at_second = lax.ppermute(at_first, "pp", [(0, 1)])
        out = jnp.where(stage == 0, at_first, jnp.where(stage == 1, at_second, jnp.where(stage == 2, at_third, out)))
        last_b = gather(out)
        last = n_micro * CHUNKS - 1
        result = store_final(result, stage, jnp.int32(last - 1), (last_a, near_a, far_a, farthest_a))
        result = store_final(result, jnp.int32(0), jnp.int32(last), (last_b,))
        return result.reshape(x_micro.shape)

    return jax.shard_map(device_fn, mesh=mesh, in_specs=in_specs, out_specs=P(), check_vma=False)
```

```python
import functools

import jax
import jax.numpy as jnp
from jax import lax
from jax.experimental import pallas as pl
from jax.experimental.pallas import tpu as pltpu
from jax.sharding import PartitionSpec as P

CHUNKS = 2
Q_BLOCK = 256
ROT_PAD = 32
LOG2E = 1.4426950408889634


def ln_kernel(stage_ref, first_ref, later_ref, gain1_ref, bias1_ref, gain2_ref, bias2_ref, attn_ref, mlp_ref):
    group, groups = 16, 8
    width = attn_ref.shape[1]

    def run(source):
        def body(index, _):
            spans = [pl.ds(pl.multiple_of((index * groups + g) * group, group), group) for g in range(groups)]
            means = [jnp.sum(source[span, :].astype(jnp.float32), axis=-1, keepdims=True) / width for span in spans]
            scales = []
            for span, mean in zip(spans, means):
                centered = source[span, :].astype(jnp.float32) - mean
                scales.append(lax.rsqrt(jnp.sum(centered * centered, axis=-1, keepdims=True) / width + 1e-5))
            for span, mean, scale in zip(spans, means, scales):
                normed = (source[span, :].astype(jnp.float32) - mean) * scale
                attn_ref[span, :] = (normed * gain1_ref[...] + bias1_ref[...]).astype(jnp.bfloat16)
                mlp_ref[span, :] = (normed * gain2_ref[...] + bias2_ref[...]).astype(jnp.bfloat16)
            return 0

        lax.fori_loop(0, attn_ref.shape[0] // (group * groups), body, 0)

    @pl.when(stage_ref[0] == 0)
    def _():
        run(first_ref.at[0])

    @pl.when(stage_ref[0] != 0)
    def _():
        run(later_ref)


def layer_norms(stage, slot, first, later, gain1, bias1, gain2, bias2):
    rows, width = later.shape
    block = 128
    scalars = jnp.stack([stage, slot]).astype(jnp.int32)
    vec = pl.BlockSpec((1, width), lambda j, s: (0, 0))
    return pl.pallas_call(
        ln_kernel,
        out_shape=[jax.ShapeDtypeStruct((rows, width), jnp.bfloat16)] * 2,
        grid_spec=pltpu.PrefetchScalarGridSpec(
            num_scalar_prefetch=1,
            grid=(rows // block,),
            in_specs=[
                pl.BlockSpec((1, block, width), lambda j, s: (s[1], jnp.where(s[0] == 0, j, 0), 0)),
                pl.BlockSpec((block, width), lambda j, s: (jnp.where(s[0] == 0, 0, j), 0)),
                vec, vec, vec, vec,
            ],
            out_specs=[pl.BlockSpec((block, width), lambda j, s: (j, 0))] * 2,
        ),
        cost_estimate=pl.CostEstimate(flops=rows * width * 600, bytes_accessed=rows * width * 6, transcendentals=0),
        name="layer_norms",
    )(scalars, first, later, gain1, bias1, gain2, bias2)


def rotate(x_t, swap, cos_t, sin_t):
    top = swap.shape[0]
    swapped = jnp.dot(swap, x_t, preferred_element_type=jnp.float32)
    mixed = x_t[:top].astype(jnp.float32) * cos_t + swapped * sin_t
    return jnp.concatenate([mixed, x_t[top:].astype(jnp.float32)], axis=0)


def attn_kernel(n_prev, *refs):
    if n_prev:
        q_ref, k_ref, v_ref, swap_ref, cos_ref, sin_ref, k_prev_ref, v_prev_ref, ctx_ref = refs
    else:
        q_ref, k_ref, v_ref, swap_ref, cos_ref, sin_ref, ctx_ref, k_out_ref = refs
    head_dim, rows = q_ref.shape[1:]
    scale = head_dim ** -0.5 * LOG2E
    q_t = rotate(q_ref[0], swap_ref[...], cos_ref[...], sin_ref[...]).astype(jnp.bfloat16)
    k_new = rotate(k_ref[0], swap_ref[...], cos_ref[...], sin_ref[...]).T.astype(jnp.bfloat16)
    if not n_prev:
        k_out_ref[0] = k_new
    causal = lax.broadcasted_iota(jnp.int32, (Q_BLOCK, Q_BLOCK), 0) <= lax.broadcasted_iota(jnp.int32, (Q_BLOCK, Q_BLOCK), 1)
    for block in range(rows // Q_BLOCK):
        lo, hi = block * Q_BLOCK, (block + 1) * Q_BLOCK
        q_blk = q_t[:, lo:hi]
        parts = []
        if n_prev:
            parts.append((k_prev_ref[0], v_prev_ref[0]))
        if lo:
            parts.append((k_new[:lo], v_ref[0, :, :lo]))
        parts.append((k_new[lo:hi], v_ref[0, :, lo:hi]))
        scores = [jnp.dot(k_part, q_blk, preferred_element_type=jnp.float32) * scale for k_part, _ in parts]
        scores[-1] = jnp.where(causal, scores[-1], -1e30)
        top = functools.reduce(jnp.maximum, [jnp.max(s, axis=0, keepdims=True) for s in scores])
        exps = [jnp.exp2(s - top) for s in scores]
        total = functools.reduce(jnp.add, [jnp.sum(e, axis=0, keepdims=True) for e in exps])
        inv = 1.0 / total
        ctx = None
        for e, (_, v_part) in zip(exps, parts):
            term = jnp.dot(v_part, (e * inv).astype(jnp.bfloat16), preferred_element_type=jnp.float32)
            ctx = term if ctx is None else ctx + term
        ctx_ref[0, :, lo:hi] = ctx.astype(jnp.bfloat16)


def attention(qkv_t, swap, cos_t, sin_t, previous):
    n_heads, head_dim, rows = qkv_t.shape[0] // 3, qkv_t.shape[1], qkv_t.shape[2]
    n_prev = previous[0].shape[1] if previous else 0
    part = lambda which: pl.BlockSpec((1, head_dim, rows), lambda h: (3 * h + which, 0, 0))
    table = pl.BlockSpec((ROT_PAD, rows), lambda h: (0, 0))
    whole = pl.BlockSpec(swap.shape, lambda h: (0, 0))
    in_specs = [part(0), part(1), part(2), whole, table, table]
    operands = [qkv_t, qkv_t, qkv_t, swap, cos_t, sin_t]
    out_shape = [jax.ShapeDtypeStruct((n_heads, head_dim, rows), jnp.bfloat16)]
    out_specs = [pl.BlockSpec((1, head_dim, rows), lambda h: (h, 0, 0))]
    if previous:
        in_specs += [pl.BlockSpec((1, n_prev, head_dim), lambda h: (h, 0, 0)), pl.BlockSpec((1, head_dim, n_prev), lambda h: (3 * h + 2, 0, 0))]
        operands += list(previous)
    else:
        out_shape.append(jax.ShapeDtypeStruct((n_heads, rows, head_dim), jnp.bfloat16))
        out_specs.append(pl.BlockSpec((1, rows, head_dim), lambda h: (h, 0, 0)))
    pairs = n_heads * rows * (n_prev + rows)
    return pl.pallas_call(
        functools.partial(attn_kernel, n_prev),
        out_shape=out_shape,
        grid=(n_heads,),
        in_specs=in_specs,
        out_specs=out_specs,
        cost_estimate=pl.CostEstimate(flops=pairs * 1000, bytes_accessed=n_heads * rows * 128 * 12, transcendentals=pairs),
        name="attention",
    )(*operands)


def qkv_kernel(w_ref, ln_ref, bias_ref, out_ref):
    acc = lax.dot_general(w_ref[...], ln_ref[...], (((1,), (1,)), ((), ())), preferred_element_type=jnp.float32)
    out_ref[...] = (acc + bias_ref[...]).astype(jnp.bfloat16)


def qkv_projection(w_t, ln, bias_t):
    features, width = w_t.shape
    rows = ln.shape[0]
    block = features // 4
    return pl.pallas_call(
        qkv_kernel,
        out_shape=jax.ShapeDtypeStruct((features, rows), jnp.bfloat16),
        grid=(features // block,),
        in_specs=[pl.BlockSpec((block, width), lambda j: (j, 0)), pl.BlockSpec((rows, width), lambda j: (0, 0)),
                  pl.BlockSpec((block, 1), lambda j: (j, 0))],
        out_specs=pl.BlockSpec((block, rows), lambda j: (j, 0)),
        cost_estimate=pl.CostEstimate(flops=2 * features * width * rows, bytes_accessed=2 * features * width, transcendentals=0),
        name="qkv_projection",
    )(w_t, ln, bias_t)


def up_kernel(ln_ref, w_ref, bias_ref, out_ref):
    hidden = jnp.dot(ln_ref[...], w_ref[...], preferred_element_type=jnp.float32) + bias_ref[...]
    out_ref[...] = (0.5 * hidden * (1.0 + lax.erf(hidden * (0.5 ** 0.5)))).astype(jnp.bfloat16)


def up_projection(ln, w_up, bias, part):
    rows, width = ln.shape
    inner = w_up.shape[1] // 2
    block = 256
    return pl.pallas_call(
        up_kernel,
        out_shape=jax.ShapeDtypeStruct((rows, inner), jnp.bfloat16),
        grid=(inner // block,),
        in_specs=[pl.BlockSpec((rows, width), lambda j: (0, 0)), pl.BlockSpec((width, block), lambda j: (0, j + part * (inner // block))),
                  pl.BlockSpec((1, block), lambda j: (0, j + part * (inner // block)))],
        out_specs=pl.BlockSpec((rows, block), lambda j: (0, j)),
        cost_estimate=pl.CostEstimate(flops=2 * inner * width * rows, bytes_accessed=2 * inner * width, transcendentals=0),
        name="up_projection",
    )(ln, w_up, bias)


def down_kernel(low_ref, high_ref, ctx_t_ref, w_low_ref, w_high_ref, w_dense_ref, out_ref, ctx_ref):
    @pl.when(pl.program_id(0) == 0)
    def _():
        ctx_ref[...] = ctx_t_ref[...].T

    attn = jnp.dot(ctx_ref[...], w_dense_ref[...], preferred_element_type=jnp.float32)
    low = jnp.dot(low_ref[...], w_low_ref[...], preferred_element_type=jnp.float32)
    high = jnp.dot(high_ref[...], w_high_ref[...], preferred_element_type=jnp.float32)
    out_ref[...] = (attn + (low + high)).astype(jnp.bfloat16)


def down_projection(low, high, ctx_t, w_down, w_dense):
    rows, inner = low.shape
    features, width = w_dense.shape
    block = 256
    return pl.pallas_call(
        down_kernel,
        out_shape=jax.ShapeDtypeStruct((rows, width), jnp.bfloat16),
        grid=(width // block,),
        in_specs=[pl.BlockSpec((rows, inner), lambda j: (0, 0)), pl.BlockSpec((rows, inner), lambda j: (0, 0)),
                  pl.BlockSpec((features, rows), lambda j: (0, 0)), pl.BlockSpec((inner, block), lambda j: (0, j)),
                  pl.BlockSpec((inner, block), lambda j: (1, j)), pl.BlockSpec((features, block), lambda j: (0, j))],
        out_specs=pl.BlockSpec((rows, block), lambda j: (0, j)),
        scratch_shapes=[pltpu.VMEM((rows, features), jnp.bfloat16)],
        cost_estimate=pl.CostEstimate(flops=2 * (2 * inner + features) * width * rows, bytes_accessed=2 * (2 * inner + features) * width, transcendentals=0),
        name="down_projection",
    )(low, high, ctx_t, w_down, w_down, w_dense)


def unwritten(shape):
    return pl.pallas_call(
        lambda out_ref: None,
        out_shape=jax.ShapeDtypeStruct(shape, jnp.bfloat16),
        out_specs=pl.BlockSpec(memory_space=pl.ANY),
        name="unwritten",
    )()


def store_kernel(sel_ref, held_ref, *refs):
    *cand_refs, out_ref, buf_ref, in_sem, out_sem = refs
    pieces, block = buf_ref.shape[:2]
    slot = sel_ref[1]

    def read(cand_ref, piece):
        return pltpu.make_async_copy(cand_ref.at[pl.ds(piece * block, block)], buf_ref.at[piece], in_sem.at[piece])

    def write(piece):
        return pltpu.make_async_copy(buf_ref.at[piece], out_ref.at[slot, pl.ds(piece * block, block)], out_sem.at[piece])

    for index, cand_ref in enumerate(cand_refs):
        @pl.when(sel_ref[0] == index)
        def _():
            for piece in range(pieces):
                read(cand_ref, piece).start()
    for piece in range(pieces):
        read(cand_refs[0], piece).wait()
        write(piece).start()
    for piece in range(pieces):
        write(piece).wait()


def store_final(result, which, slot, candidates):
    rows, width = candidates[0].shape
    pieces = 4
    hbm = pl.BlockSpec(memory_space=pltpu.HBM)
    scalars = jnp.stack([which, slot]).astype(jnp.int32)
    return pl.pallas_call(
        store_kernel,
        out_shape=jax.ShapeDtypeStruct(result.shape, result.dtype),
        in_specs=[pl.BlockSpec(memory_space=pltpu.SMEM)] + [hbm] * (1 + len(candidates)),
        out_specs=hbm,
        scratch_shapes=[pltpu.VMEM((pieces, rows // pieces, width), result.dtype),
                        pltpu.SemaphoreType.DMA((pieces,)), pltpu.SemaphoreType.DMA((pieces,))],
        input_output_aliases={1: 0},
        cost_estimate=pl.CostEstimate(flops=rows * width * 300, bytes_accessed=rows * width * 4, transcendentals=0),
        name="store_final",
    )(scalars, result, *candidates)


def rotary_tables(seq_len, rot_dims, head_dim):
    half = rot_dims // 2
    inv_freq = 1.0 / (10000.0 ** (jnp.arange(0, rot_dims, 2).astype(jnp.float32) / rot_dims))
    angles = inv_freq[:, None] * jnp.arange(seq_len).astype(jnp.float32)[None, :]
    spare = ROT_PAD - rot_dims
    cos_t = jnp.concatenate([jnp.cos(angles), jnp.cos(angles), jnp.ones((spare, seq_len), jnp.float32)])
    sin_t = jnp.concatenate([jnp.sin(angles), jnp.sin(angles), jnp.zeros((spare, seq_len), jnp.float32)])
    row = lax.broadcasted_iota(jnp.int32, (ROT_PAD, head_dim), 0)
    col = lax.broadcasted_iota(jnp.int32, (ROT_PAD, head_dim), 1)
    minus = jnp.logical_and(row < half, col == row + half)
    plus = jnp.logical_and(jnp.logical_and(row >= half, row < rot_dims), col == row - half)
    swap = jnp.where(plus, 1.0, jnp.where(minus, -1.0, 0.0)).astype(jnp.bfloat16)
    return swap, cos_t, sin_t


def solution(mesh):
    n_stages, n_tp = mesh.shape["pp"], mesh.shape["tp"]
    in_specs = (P(), P("pp", None), P("pp", None), P("pp", None, "tp", None), P("pp", "tp", None),
                P("pp", "tp", None, None), P("pp", None), P("pp", None), P("pp", None),
                P("pp", None, "tp"), P("pp", "tp"), P("pp", "tp", None), P("pp", None))

    def device_fn(x_micro, ln1_gain, ln1_bias, w_qkv, b_qkv, w_dense, b_dense, ln2_gain, ln2_bias, w_up, b_up, w_down, b_down):
        n_micro, _, seq_len, width = x_micro.shape
        n_heads, head_dim = w_dense.shape[1:3]
        rows = seq_len // CHUNKS
        quarter = rows // n_tp
        stage, tp_id = lax.axis_index("pp"), lax.axis_index("tp")
        x_chunks = x_micro.reshape(n_micro * CHUNKS, rows, width)
        norms = [v[:1].astype(jnp.float32) for v in (ln1_gain, ln1_bias, ln2_gain, ln2_bias)]
        bias_sum = b_dense[0].astype(jnp.float32) + b_down[0].astype(jnp.float32)
        w_qkv_t = w_qkv[0].transpose(1, 2, 0).reshape(n_heads * 3 * head_dim, width)
        b_qkv_t = b_qkv[0].reshape(n_heads * 3 * head_dim, 1).astype(jnp.float32)
        w_qkv_t, b_qkv_t = lax.optimization_barrier((w_qkv_t, b_qkv_t))
        w_out = w_dense[0].reshape(n_heads * head_dim, width)
        up_bias = b_up[:1].astype(jnp.float32)
        swap, cos_t, sin_t = rotary_tables(seq_len, head_dim // 4, head_dim)
        tables = [(cos_t[:, c * rows:(c + 1) * rows], sin_t[:, c * rows:(c + 1) * rows]) for c in range(CHUNKS)]
        swap, tables = lax.optimization_barrier((swap, tables))
        ring = [(s, (s + 1) % n_stages) for s in range(n_stages)]

        def norms_of(chunk, slot, gathered):
            where_from = slot * CHUNKS + chunk
            ln_attn, ln_mlp = layer_norms(stage, where_from, x_chunks, gathered, *norms)
            from_x = lax.dynamic_slice(x_chunks, (where_from, tp_id * quarter, 0), (1, quarter, width))[0]
            from_ring = lax.dynamic_slice(gathered, (tp_id * quarter, 0), (quarter, width))
            return ln_attn, ln_mlp, jnp.where(stage == 0, from_x, from_ring)

        def attend(chunk, ln_attn, previous):
            qkv_t = qkv_projection(w_qkv_t, ln_attn, b_qkv_t).reshape(3 * n_heads, head_dim, rows)
            if previous is None:
                ctx_t, keys = attention(qkv_t, swap, *tables[chunk], None)
                previous = (keys, qkv_t)
            else:
                ctx_t, = attention(qkv_t, swap, *tables[chunk], previous)
            return ctx_t.reshape(n_heads * head_dim, rows), previous

        def scatter(partial):
            return lax.psum_scatter(partial, "tp", scatter_dimension=0, tiled=True)

        def pass_on(summed, kept):
            out = (kept.astype(jnp.float32) + bias_sum + summed.astype(jnp.float32)).astype(jnp.bfloat16)
            return lax.ppermute(out, "pp", ring)

        def gather(out):
            return lax.all_gather(out, "tp", axis=0, tiled=True)

        def to_far(final):
            return lax.ppermute(final, "pp", [(0, 2)])

        def to_near(final):
            return lax.ppermute(final, "pp", [(0, 1)])

        def to_third(far):
            return lax.ppermute(far, "pp", [(2, 3)])

        def half(chunk, slot, done, gathered, previous, partial_before, kept_before, result):
            summed = scatter(partial_before)
            far = to_far(gathered)
            ln_attn, ln_mlp, kept = norms_of(chunk, slot, gathered)
            ctx_t, previous = attend(chunk, ln_attn, previous)
            summed, far, ctx_t, ln_mlp, kept = lax.optimization_barrier((summed, far, ctx_t, ln_mlp, kept))
            passed = pass_on(summed, kept_before)
            high = up_projection(ln_mlp, w_up[0], up_bias, 1)
            passed, high, far, ln_mlp, gathered = lax.optimization_barrier((passed, high, far, ln_mlp, gathered))
            gathered_before = gather(passed)
            near, farthest = to_near(gathered), to_third(far)
            low = up_projection(ln_mlp, w_up[0], up_bias, 0)
            low, near, farthest = lax.optimization_barrier((low, near, farthest))
            result = store_final(result, stage, done * CHUNKS + chunk, (gathered, near, far, farthest))
            partial = down_projection(low, high, ctx_t, w_down[0], w_out)
            gathered_before, partial, result = lax.optimization_barrier((gathered_before, partial, result))
            return gathered_before, partial, kept, previous, result

        def tick(step, carry):
            gathered_a, partial_b, kept_b, result = carry
            slot = jnp.clip(step, 0, n_micro - 1)
            done = jnp.maximum(step - n_stages, 0)
            gathered_b, partial_a, kept_a, previous, result = half(0, slot, done, gathered_a, None, partial_b, kept_b, result)
            next_a, partial_b, kept_b, _, result = half(1, slot, done, gathered_b, previous, partial_a, kept_a, result)
            return next_a, partial_b, kept_b, result

        start = (x_chunks[0], x_chunks[1], x_chunks[0, :quarter], unwritten(x_chunks.shape))
        last_a, partial_b, kept_b, result = lax.fori_loop(0, n_micro + n_stages - 1, tick, start)
        summed = scatter(partial_b)
        far_a, near_a = to_far(last_a), to_near(last_a)
        summed, far_a, near_a = lax.optimization_barrier((summed, far_a, near_a))
        out = (kept_b.astype(jnp.float32) + bias_sum + summed.astype(jnp.float32)).astype(jnp.bfloat16)
        at_first = lax.ppermute(out, "pp", [(n_stages - 1, 0)])
        at_third = lax.ppermute(out, "pp", [(n_stages - 1, 2)])
        farthest_a = to_third(far_a)
        at_second = lax.ppermute(at_first, "pp", [(0, 1)])
        out = jnp.where(stage == 0, at_first, jnp.where(stage == 1, at_second, jnp.where(stage == 2, at_third, out)))
        last_b = gather(out)
        last = n_micro * CHUNKS - 1
        result = store_final(result, stage, jnp.int32(last - 1), (last_a, near_a, far_a, farthest_a))
        result = store_final(result, jnp.int32(0), jnp.int32(last), (last_b,))
        return result.reshape(x_micro.shape)

    return jax.shard_map(device_fn, mesh=mesh, in_specs=in_specs, out_specs=P(), check_vma=False)
```
